32 devices in a mesh: dp: 16 (over z, y, x), mp: 2 (over core).
Axes of the slice: x: 2, y: 2, z: 4, core: 2. Of those that a mesh axis runs over, the one named last changes fastest.
Arguments:
- embeddings: float32 [12288, 1024], P('dp', 'mp')
- cluster_id: int32 [12288], P('dp'), may hold values from 0 to 4095, as said below
- centroids: float32 [4096, 1024], P('dp', 'mp'), may hold values from -6 to 6
- cluster_mass: float32 [4096], P('dp'), may hold values from 1 to 16
Outputs:
- max_similarity: float32 [12288], P('dp')
- new_centroids: float32 [4096, 1024], P('dp', 'mp')
The draws below stay inside these ranges and needn't reach their ends.
Inputs may be any that keep to these rules, and one draw needn't show every extreme that they name: `cluster_id`: cluster k belongs to owner k // 256. Among the 768 rows of one index of dp, at most 96 have clusters of any one owner, and for some owner exactly 96.
All inputs are finite; a program needn't handle non-finite values.
Results may differ from the reference program's by a relative error of at most 0.0011.
Values may be sent and summed in bfloat16 or wider, within the bound.
No kernel may reach another device: no remote copies, remote signals or barrier semaphores. Data moves between devices by JAX's collectives and lax.ppermute only.
A program may use at most 64 MiB of HBM per device.

```python
import math
import jax
import jax.numpy as jnp
from jax import lax

D = 1024
CL_DEV = 256
ROW_DEV = 768
CLUSTERS = 4096
ROWS = 12288
CAP = 96


def cluster_helper(key):
    owners = ROWS // ROW_DEV
    base = jax.random.fold_in(key, 3)

    def one_block(block_key):
        first, second, third, fourth = jax.random.split(block_key, 4)
        full_owner = jax.random.randint(first, (), 0, owners)
        others = (full_owner + 1 + jnp.arange((owners - 1) * CAP) // CAP) % owners
        order = jax.random.permutation(second, (owners - 1) * CAP)
        picks = others[order[:ROW_DEV - CAP]]
        chosen = jnp.concatenate([jnp.full((CAP,), full_owner), picks])
        chosen = chosen[jax.random.permutation(third, ROW_DEV)]
        local = jax.random.randint(fourth, (ROW_DEV,), 0, CL_DEV)
        return (chosen * CL_DEV + local).astype(jnp.int32)
    keys = jax.random.split(base, owners)
    return jax.vmap(one_block)(keys).reshape(ROWS)


def draw_cluster_id(key, part):
    return cluster_helper(key)


def draw_embeddings(key, part):
    ids = cluster_helper(key)
    centre_key = jax.random.fold_in(key, 7)
    centres = jax.vmap(lambda ident: jax.random.normal(jax.random.fold_in(centre_key, ident), (D,), jnp.float32))(ids)
    noise_key = jax.random.fold_in(key, 11)
    noise = jax.random.normal(noise_key, (ROWS, D), jnp.float32)
    values = 0.8 * centres + 0.6 * noise
    return values.astype(jnp.float32)


def level_of(rng, dims, pieces, smallest, top_value):
    level, own = 1.0, jax.random.fold_in(rng, 6)
    for dim, blocks in pieces:
        heights = jnp.exp(jax.random.uniform(jax.random.fold_in(own, dim), (blocks,), jnp.float32, smallest / len(pieces), top_value / len(pieces)))
        level = level * jnp.repeat(heights, dims[dim] // blocks).reshape([-1 if axis == dim else 1 for axis in range(len(dims))])
    return level


def scatter_about(stream_key, dims, scale, bound, shards=(), kind=jnp.bfloat16):
    gain = level_of(stream_key, dims, shards, -0.22, 0.18) if shards else 1.0
    values = jax.random.normal(stream_key, dims, jnp.float32) * scale * gain
    return jnp.minimum(jnp.maximum(values, -bound), bound).astype(kind)


def setup_inputs(seed: int = 0) -> dict:
    key_of = jax.random.split(jax.random.key(seed), 5)
    embeddings = draw_embeddings(jax.random.fold_in(key_of[4], 71), 0)
    cluster_id = draw_cluster_id(jax.random.fold_in(key_of[4], 71), 0)
    centroids = scatter_about(key_of[2], (CLUSTERS, D), 1.0, 6.0, ((0, 16), (1, 2)), jnp.float32)
    cluster_mass = jnp.clip(jnp.exp(math.log(16.0) - 2.7725887 * jax.random.uniform(key_of[3], (CLUSTERS,), jnp.float32) ** level_of(key_of[3], (CLUSTERS,), ((0, 16),), -0.2, 0.2)), 1.0, 16.0)
    return dict(embeddings=embeddings, cluster_id=cluster_id, centroids=centroids, cluster_mass=cluster_mass)


def reference(embeddings, cluster_id, centroids, cluster_mass):
    owners = ROWS // ROW_DEV
    slots = 2 * ROW_DEV
    cap = slots // owners
    squares = lax.optimization_barrier(jnp.sum(embeddings * embeddings, axis=1))
    unit = (embeddings * lax.rsqrt(squares / D + 1e-06)[:, None]).astype(jnp.bfloat16)
    owner = (cluster_id // CL_DEV).astype(jnp.int32)
    local = (cluster_id - owner * CL_DEV).astype(jnp.int32)
    sums = jnp.zeros((CLUSTERS, D), jnp.float32).at[cluster_id].add(unit.astype(jnp.float32))
    counts = jnp.zeros((CLUSTERS,), jnp.float32).at[cluster_id].add(jnp.ones((ROWS,), jnp.float32))
    new_centroids = (cluster_mass[:, None] * centroids + sums) / (cluster_mass + counts)[:, None]
    blocked = owner.reshape(owners, ROW_DEV)
    hot = (blocked[:, :, None] == jnp.arange(owners, dtype=jnp.int32)[None, None, :]).astype(jnp.int32)
    running = jnp.cumsum(hot, axis=1)
    rank = jnp.take_along_axis(running, blocked[:, :, None], axis=2)[:, :, 0] - 1
    source = (jnp.arange(ROWS, dtype=jnp.int32) // ROW_DEV).astype(jnp.int32)
    position = (source * cap + rank.reshape(ROWS)).astype(jnp.int32)
    buffer = jnp.zeros((owners, slots, D), jnp.bfloat16).at[owner, position].set(unit)
    bids = jnp.full((owners, slots), -1, jnp.int32).at[owner, position].set(local)

    def one_owner(pair):
        rows, ids = pair
        wide = rows.astype(jnp.float32)
        scores = jnp.dot(wide, wide.T, precision=lax.Precision.HIGHEST) / D
        index = jnp.arange(slots, dtype=jnp.int32)
        same = (ids[:, None] == ids[None, :]) & (ids[:, None] >= 0) & (index[:, None] != index[None, :])
        return lax.optimization_barrier(jnp.max(jnp.where(same, scores, -1.0), axis=1))
    best = lax.map(one_owner, (buffer, bids))
    max_similarity = best[owner, position]
    return (max_similarity, new_centroids)
```

```python
import jax
import jax.numpy as jnp
from jax import lax
from jax.sharding import PartitionSpec as P

D = 1024


def swap_cores(value):
    size = lax.axis_size("mp")
    return lax.ppermute(value, "mp", [(i, (i + 1) % size) for i in range(size)])


def shards(embeddings, cluster_id, centroids, cluster_mass):
    owners = lax.axis_size("dp")
    row_count = embeddings.shape[0]
    slot_count = 2 * row_count
    capacity = slot_count // owners
    cluster_count = centroids.shape[0]
    owner = cluster_id // cluster_count
    local = cluster_id - owner * cluster_count
    partial = jnp.sum(embeddings * embeddings, axis=1)
    squares = partial + swap_cores(partial)
    unit = (embeddings * lax.rsqrt(squares / D + 1e-06)[:, None]).astype(jnp.bfloat16)
    owner_hot = (owner[:, None] == jnp.arange(owners, dtype=jnp.int32)[None, :]).astype(
        jnp.bfloat16
    )
    row_index = jnp.arange(row_count, dtype=jnp.int32)
    lower = (row_index[:, None] >= row_index[None, :]).astype(jnp.bfloat16)
    running = jnp.dot(lower, owner_hot, preferred_element_type=jnp.float32)
    rank = jnp.sum(running * owner_hot.astype(jnp.float32), axis=1).astype(jnp.int32) - 1
    slot = owner * capacity + rank
    slot_index = jnp.arange(slot_count, dtype=jnp.int32)
    placed = slot_index[:, None] == slot[None, :]
    out_ids = jnp.max(jnp.where(placed, local[None, :] + 1, 0), axis=1) - 1
    outgoing = jnp.dot(
        placed.astype(jnp.bfloat16), unit, preferred_element_type=jnp.float32
    ).astype(jnp.bfloat16)
    incoming = lax.all_to_all(outgoing, "dp", split_axis=0, concat_axis=0, tiled=True)
    in_ids = lax.all_to_all(out_ids, "dp", split_axis=0, concat_axis=0, tiled=True)
    other = swap_cores(incoming)
    member = (jnp.arange(cluster_count, dtype=jnp.int32)[:, None] == in_ids[None, :]).astype(
        jnp.bfloat16
    )
    sums = jnp.dot(member, incoming, preferred_element_type=jnp.float32)
    counts = jnp.sum(member.astype(jnp.float32), axis=1)
    new_centroids = (cluster_mass[:, None] * centroids + sums) / (cluster_mass + counts)[:, None]
    half = slot_count // 2
    start = lax.axis_index("mp") * half
    contract = (((1,), (1,)), ((), ()))
    gathered = jnp.concatenate([incoming, other], axis=1)
    queries = lax.dynamic_slice_in_dim(gathered, start, half, 0)
    scores = lax.dot_general(queries, gathered, contract, preferred_element_type=jnp.float32)
    scores = scores / D
    query_ids = lax.dynamic_slice_in_dim(in_ids, start, half, 0)
    query_pos = start + jnp.arange(half, dtype=jnp.int32)
    same = (
        (query_ids[:, None] == in_ids[None, :])
        & (query_ids[:, None] >= 0)
        & (query_pos[:, None] != slot_index[None, :])
    )
    best = jnp.max(jnp.where(same, scores, -1.0), axis=1)
    partner = swap_cores(best)
    first = lax.axis_index("mp") == 0
    best_all = jnp.concatenate([jnp.where(first, best, partner), jnp.where(first, partner, best)])
    returned = lax.all_to_all(best_all, "dp", split_axis=0, concat_axis=0, tiled=True)
    max_similarity = jnp.max(jnp.where(placed, returned[:, None], -2.0), axis=0)
    return (max_similarity, new_centroids)


def solution(mesh):
    in_specs = (P("dp", "mp"), P("dp"), P("dp", "mp"), P("dp"))
    out_specs = (P("dp"), P("dp", "mp"))
    return jax.shard_map(shards, mesh=mesh, in_specs=in_specs, out_specs=out_specs, check_vma=False)
```
